32 devices in a mesh: dev: 32 (over z, y, x, core).
Axes of the slice: x: 2, y: 2, z: 4, core: 2. Of those that a mesh axis runs over, the one named last changes fastest.
Arguments:
- source: bfloat16 [48, 262144], P(None, 'dev'), may hold values from -6 to 6
- weights: bfloat16 [20480, 128, 128], P('dev'), may hold values from -0.01953125 to 0.01953125
- tile_map: int32 [3, 20480], P(None, 'dev'), may hold values from 0 to 63, as said below
- tile_count: int32 [32], P('dev'), may hold values from 160 to 640, as said below
Outputs:
- acoustic_source: float32 [48, 4096], P(None, 'dev')
The draws below stay inside these ranges and needn't reach their ends.
Inputs may be any that keep to these rules, and one draw needn't show every extreme that they name: `tile_map`: row 0 is a CFD block of the owning device; row 2 an acoustic block of the destination. Row 1 is a device at cyclic distance at most 4 from the owner in device order, or at distance exactly 32 // 2 (counted upward); every device has used slots at distance +4, -4 and 32 // 2. `tile_count`: some device uses all its slots.
All inputs are finite; a program needn't handle non-finite values.
Results may differ from the reference program's by a relative error of at most 0.0003.
Values sent between devices are 32-bit elements; how exact they have to be, the bound alone decides.
No kernel may reach another device: no remote copies, remote signals or barrier semaphores. Data moves between devices by JAX's collectives and lax.ppermute only.
A program may use at most 128 MiB of HBM per device.

```python
import jax
import jax.numpy as jnp
from jax import lax

BLK = 128
REACH = 4
SRC_BLK_DEV = 64
TILES_DEV = 640
ACU_BLK_DEV = 1
FEAT = 48
CELLS = 262144
TILES = 20480
N_DEV = 32


def draw_tile_map(key, part):
    key_src = jax.random.fold_in(key, 11)
    key_off = jax.random.fold_in(key, 12)
    key_blk = jax.random.fold_in(key, 13)
    total = N_DEV * TILES_DEV
    src_ids = jax.random.randint(key_src, (total,), 0, SRC_BLK_DEV)
    offsets = jax.random.randint(key_off, (total,), -REACH, REACH + 1)
    slot = jnp.arange(total) % TILES_DEV
    offsets = jnp.where(slot == 0, REACH, jnp.where(slot == 1, -REACH, jnp.where(slot == 2, N_DEV // 2, offsets)))
    owner = jnp.arange(total) // TILES_DEV
    dest = (owner + offsets) % N_DEV
    dest_blk = jax.random.randint(key_blk, (total,), 0, ACU_BLK_DEV)
    return jnp.stack([src_ids, dest, dest_blk]).astype(jnp.int32)


def draw_tile_count(key, part):
    key_cnt = jax.random.fold_in(key, 21)
    key_full = jax.random.fold_in(key, 22)
    lowest = max(TILES_DEV // 4, 3)
    counts = jax.random.randint(key_cnt, (N_DEV,), lowest, TILES_DEV + 1)
    busiest = jax.random.randint(key_full, (), 0, N_DEV)
    counts = jnp.where(jnp.arange(N_DEV) == busiest, TILES_DEV, counts)
    return counts.astype(jnp.int32)


def block_scale(own_key, shape, cuts, low, high):
    level = 1.0
    for position, shards_of in cuts:
        steps = jax.random.uniform(jax.random.fold_in(jax.random.fold_in(own_key, 6), position), (shards_of,), jnp.float32, low / len(cuts), high / len(cuts))
        level = level * jnp.repeat(jnp.exp(steps), shape[position] // shards_of).reshape((-1,) + (1,) * (len(shape) - 1 - position))
    return level


def centred(own_key, dims, scale, most, split=(), kind=jnp.bfloat16):
    drawn = jax.random.normal(own_key, dims, jnp.float32) * scale
    if len(split) > 0:
        drawn = block_scale(own_key, dims, split, -0.22, 0.18) * drawn
    return jnp.clip(drawn, min=-most, max=most).astype(kind)


def setup_inputs(seed: int = 0) -> dict:
    splits = jax.random.split(jax.random.key(seed), 5)
    source = centred(splits[0], (FEAT, CELLS), 1.0, 6.0, ((1, 32),))
    weights = centred(splits[1], (TILES, BLK, BLK), (BLK * TILES_DEV // ACU_BLK_DEV) ** -0.5, 0.01953125, ((0, 32),))
    tile_map = draw_tile_map(jax.random.fold_in(splits[4], 71), 0)
    tile_count = draw_tile_count(jax.random.fold_in(splits[4], 71), 0)
    return dict(source=source, weights=weights, tile_map=tile_map, tile_count=tile_count)


def reference(source, weights, tile_map, tile_count):
    feat = source.shape[0]
    blocks = source.reshape(feat, N_DEV * SRC_BLK_DEV, BLK).astype(jnp.float32)

    def one_device(acc, device):
        start = device * TILES_DEV
        tile_w = lax.dynamic_slice_in_dim(weights, start, TILES_DEV, 0).astype(jnp.float32)
        mapped = lax.dynamic_slice_in_dim(tile_map, start, TILES_DEV, 1)
        block_ids = (device * SRC_BLK_DEV + mapped[0]).astype(jnp.int32)
        picked = jnp.take(blocks, block_ids, axis=1)
        product = jnp.einsum("ftc,tcn->tfn", picked, tile_w, precision=lax.Precision.HIGHEST)
        used = (jnp.arange(TILES_DEV, dtype=jnp.int32) < tile_count[device]).astype(jnp.float32)
        product = product * used[:, None, None]
        target = (mapped[1] * ACU_BLK_DEV + mapped[2]).astype(jnp.int32)
        return acc.at[target].add(product), None

    start_acc = jnp.zeros((N_DEV * ACU_BLK_DEV, feat, BLK), jnp.float32)
    acc, _ = lax.scan(one_device, start_acc, jnp.arange(N_DEV, dtype=jnp.int32))
    return jnp.transpose(acc, (1, 0, 2)).reshape(feat, N_DEV * ACU_BLK_DEV * BLK)
```

```python
import functools

import jax
import jax.numpy as jnp
from jax import lax
from jax.experimental import pallas as pl
from jax.experimental.pallas import tpu as pltpu
from jax.sharding import PartitionSpec as P

REACH = 4
ACU_BLK_DEV = 1
GROUP = 64


def passed_along(value, axis, steps):
    count = lax.axis_size(axis)
    pairs = [(source, (source + steps) % count) for source in range(count)]
    return lax.ppermute(value, axis, pairs)


def tile_kernel(devices, acu, offsets, group, map_hbm, count_hbm, source_hbm, weights_hbm, *rest):
    outs, scratch = rest[: len(offsets)], rest[len(offsets) :]
    tile_map, tile_count, source, weights, even, odd, map_sem, count_sem, source_sem, weight_sems = scratch
    tiles, blk = weights_hbm.shape[0], weights_hbm.shape[1]
    groups = tiles // group
    spare = devices * acu

    def chunk(index):
        start = index * group
        return pltpu.make_async_copy(weights_hbm.at[pl.ds(start, group)], weights.at[pl.ds(start, group)], weight_sems.at[index])

    count_copy = pltpu.make_async_copy(count_hbm, tile_count, count_sem)
    map_copy = pltpu.make_async_copy(map_hbm, tile_map, map_sem)
    source_copy = pltpu.make_async_copy(source_hbm, source, source_sem)
    count_copy.start()
    map_copy.start()
    source_copy.start()
    chunk(0).start()
    own = lax.axis_index("dev")

    def slot(offset):
        return lax.rem(own + offset + devices, devices) * acu

    for offset_list in offsets:
        for offset in offset_list:
            for part in range(acu):
                for total in (even, odd):
                    total[slot(offset) + part] = jnp.zeros(total.shape[1:], total.dtype)
    count_copy.wait()
    used = tile_count[0]
    for index in range(1, groups):
        @pl.when(index * group < used)
        def _():
            chunk(index).start()
    map_copy.wait()
    source_copy.wait()

    def one_group(index, carry):
        chunk(index).wait()
        for pair in range(group // 2):
            left, right = [], []
            for side in range(2):
                tile = index * group + 2 * pair + side
                block = pl.multiple_of(tile_map[0, tile] * blk, blk)
                left.append(source[:, pl.ds(block, blk)])
                right.append(weights[tile])
            product = jnp.dot(jnp.concatenate(left, 0), jnp.concatenate(right, 1), preferred_element_type=jnp.float32)
            feat = left[0].shape[0]
            for side, total in enumerate((even, odd)):
                tile = index * group + 2 * pair + side
                target = jnp.where(tile < used, tile_map[1, tile] * acu + tile_map[2, tile], spare)
                total[target] += product[side * feat : (side + 1) * feat, side * blk : (side + 1) * blk]
        return carry

    lax.fori_loop(0, pl.cdiv(used, group), one_group, 0)
    for out, offset_list in zip(outs, offsets):
        for place, offset in enumerate(offset_list):
            for part in range(acu):
                out[place * acu + part] = even[slot(offset) + part] + odd[slot(offset) + part]


def on_device(source, weights, tile_map, tile_count):
    feat, cells = source.shape
    tiles, blk = weights.shape[0], weights.shape[1]
    acu = ACU_BLK_DEV
    devices = lax.axis_size("dev")
    half_way = devices // 2
    offsets = [(2, 3, 4), (-4, -3, -2), (-1, 0, 1)]
    has_far = half_way > REACH
    if has_far:
        offsets.append((half_way,))
    group = next(g for g in range(GROUP, 0, -2) if tiles % g == 0)
    acc = pltpu.VMEM((devices * acu + 1, feat, blk), jnp.float32)
    results = pl.pallas_call(
        functools.partial(tile_kernel, devices, acu, offsets, group),
        out_shape=[jax.ShapeDtypeStruct((len(o) * acu, feat, blk), jnp.float32) for o in offsets],
        in_specs=[pl.BlockSpec(memory_space=pltpu.HBM)] * 4,
        out_specs=[pl.BlockSpec(memory_space=pltpu.VMEM)] * len(offsets),
        scratch_shapes=[
            pltpu.SMEM(tile_map.shape, jnp.int32),
            pltpu.SMEM(tile_count.shape, jnp.int32),
            pltpu.VMEM(source.shape, source.dtype),
            pltpu.VMEM(weights.shape, weights.dtype),
            acc,
            acc,
            pltpu.SemaphoreType.DMA,
            pltpu.SemaphoreType.DMA,
            pltpu.SemaphoreType.DMA,
            pltpu.SemaphoreType.DMA((tiles // group,)),
        ],
        compiler_params=pltpu.CompilerParams(vmem_limit_bytes=48 * 1024 * 1024),
    )(tile_map, tile_count, source, weights)
    up, down, near = results[:3]
    near = near + passed_along(up, "dev", 3) + passed_along(down, "dev", -3)
    below, mine, above = near[:acu], near[acu : 2 * acu], near[2 * acu :]
    total = mine
    if has_far:
        total = total + passed_along(results[3], "dev", half_way)
    total = total + passed_along(below, "dev", -1) + passed_along(above, "dev", 1)
    return jnp.transpose(total, (1, 0, 2)).reshape(feat, acu * blk)


def solution(mesh):
    return jax.shard_map(
        on_device,
        mesh=mesh,
        in_specs=(P(None, "dev"), P("dev", None, None), P(None, "dev"), P("dev")),
        out_specs=P(None, "dev"),
        check_vma=False,
    )
```

```python
import functools

import jax
import jax.numpy as jnp
from jax import lax
from jax.experimental import pallas as pl
from jax.experimental.pallas import tpu as pltpu
from jax.sharding import PartitionSpec as P

REACH = 4
ACU_BLK_DEV = 1
GROUP = 80
VMEM_LIMIT = 66000000


def sent(value, target):
    count = lax.axis_size("dev")
    return lax.ppermute(value, "dev", [(source, target(source) % count) for source in range(count)])


def pair_device(own, pairs, side, devices):
    return lax.rem(own // 2 + pairs + devices, devices // 2) * 2 + side


def outward(own, devices):
    odd = lax.rem(own, 2)
    step = 1 - 2 * odd
    return [pair_device(own, step * far, odd ^ flip, devices) for far in range(1, REACH // 2 + 1) for flip in (0, 1)]


def handed_over(own, devices):
    odd = lax.rem(own, 2)
    step = 2 * odd - 1
    return [pair_device(own, step * far, odd ^ 1 ^ flip, devices) for far in range(1, REACH // 2 + 1) for flip in (0, 1)]


def half_way(own, devices):
    return [lax.rem(own + devices // 2, devices)]


def kept(own, devices):
    return [own, own ^ 1]


def tile_kernel(devices, acu, slots, group, map_hbm, count_hbm, source_hbm, weights_hbm, *rest):
    outs, scratch = rest[: len(slots)], rest[len(slots) :]
    tile_map, tile_count, source, weights, even, odd, map_sem, count_sem, source_sem, weight_sems = scratch
    tiles, blk = weights_hbm.shape[0], weights_hbm.shape[1]
    groups = tiles // group
    spare = devices * acu

    def chunk(index):
        span = pl.ds(index * group, group)
        return pltpu.make_async_copy(weights_hbm.at[span], weights.at[span], weight_sems.at[index])

    count_copy = pltpu.make_async_copy(count_hbm, tile_count, count_sem)
    map_copy = pltpu.make_async_copy(map_hbm, tile_map, map_sem)
    source_copy = pltpu.make_async_copy(source_hbm, source, source_sem)
    count_copy.start()
    map_copy.start()
    source_copy.start()
    chunk(0).start()
    own = lax.axis_index("dev")
    for targets in slots:
        for target in targets(own, devices):
            for part in range(acu):
                for total in (even, odd):
                    total[target * acu + part] = jnp.zeros(total.shape[1:], total.dtype)
    count_copy.wait()
    used = tile_count[0]
    for index in range(1, groups):
        @pl.when(index * group < used)
        def _():
            chunk(index).start(priority=1)
    map_copy.wait()
    source_copy.wait()

    def one_group(index, carry):
        chunk(index).wait()
        for pair in range(group // 2):
            left, right = [], []
            for side in range(2):
                tile = index * group + 2 * pair + side
                block = pl.multiple_of(tile_map[0, tile] * blk, blk)
                left.append(source[:, pl.ds(block, blk)])
                right.append(weights[tile])
            product = jnp.dot(jnp.concatenate(left, 0), jnp.concatenate(right, 1), preferred_element_type=jnp.float32)
            feat = left[0].shape[0]
            for side, total in enumerate((even, odd)):
                tile = index * group + 2 * pair + side
                target = jnp.where(tile < used, tile_map[1, tile] * acu + tile_map[2, tile], spare)
                total[target] += product[side * feat : (side + 1) * feat, side * blk : (side + 1) * blk]
        return carry

    lax.fori_loop(0, pl.cdiv(used, group), one_group, 0)
    for out, targets in zip(outs, slots):
        for place, target in enumerate(targets(own, devices)):
            for part in range(acu):
                out[place * acu + part] = even[target * acu + part] + odd[target * acu + part]


def on_device(source, weights, tile_map, tile_count):
    feat = source.shape[0]
    tiles, blk = weights.shape[0], weights.shape[1]
    acu = ACU_BLK_DEV
    devices = lax.axis_size("dev")
    slots = [outward, handed_over, kept, half_way]
    sizes = [REACH * acu, REACH * acu, 2 * acu, acu]
    group = next(g for g in range(GROUP, 0, -2) if tiles % g == 0)
    sums = pltpu.VMEM((devices * acu + 1, feat, blk), jnp.float32)
    out, handed, mine, far = pl.pallas_call(
        functools.partial(tile_kernel, devices, acu, slots, group),
        out_shape=[pltpu.VMEM((size, feat, blk), jnp.float32) for size in sizes],
        in_specs=[pl.BlockSpec(memory_space=pltpu.HBM)] * 4,
        out_specs=[pl.BlockSpec(memory_space=pltpu.VMEM)] * len(slots),
        scratch_shapes=[
            pltpu.SMEM(tile_map.shape, jnp.int32),
            pltpu.SMEM(tile_count.shape, jnp.int32),
            pltpu.VMEM(source.shape, source.dtype),
            pltpu.VMEM(weights.shape, weights.dtype),
            sums,
            sums,
            pltpu.SemaphoreType.DMA,
            pltpu.SemaphoreType.DMA,
            pltpu.SemaphoreType.DMA,
            pltpu.SemaphoreType.DMA((tiles // group,)),
        ],
        compiler_params=pltpu.CompilerParams(vmem_limit_bytes=VMEM_LIMIT),
    )(tile_map, tile_count, source, weights)
    out = out + sent(handed, lambda d: d ^ 1)
    for far_pairs in range(1, REACH // 2 + 1):
        piece = out[2 * (far_pairs - 1) * acu : 2 * far_pairs * acu]
        mine = mine + sent(piece, lambda d: d + 2 * far_pairs * (1 - 2 * (d % 2)))
    far = sent(far, lambda d: d + devices // 2)
    total = mine[:acu] + far + sent(mine[acu:], lambda d: d ^ 1)
    return jnp.transpose(total, (1, 0, 2)).reshape(feat, acu * blk)


def solution(mesh):
    return jax.shard_map(
        on_device,
        mesh=mesh,
        in_specs=(P(None, "dev"), P("dev", None, None), P(None, "dev"), P("dev")),
        out_specs=P(None, "dev"),
        check_vma=False,
    )
```
